32 devices in a mesh: leaf: 4 (over x, core), blk: 8 (over z, y).
Axes of the slice: x: 2, y: 2, z: 4, core: 2. Of those that a mesh axis runs over, the one named last changes fastest.
Arguments:
- right_side: float32 [4, 4, 8, 384], P(None, 'leaf', 'blk'), may hold values from -6 to 6
- diag_inverse: bfloat16 [4, 8, 128, 7168], P('leaf', 'blk'), as said below
- update_factor: bfloat16 [4, 8, 128, 10240], P('leaf', 'blk'), may hold values from -0.09375 to 0.09375
- live_blocks: int32 [7], replicated, may hold values from 1 to 32, as said below
Outputs:
- forward_solution: float32 [4, 4, 8, 384], P(None, 'leaf', 'blk')
- solution: float32 [4, 4, 8, 384], P(None, 'leaf', 'blk')
The draws below stay inside these ranges and needn't reach their ends.
Inputs may be any that keep to these rules, and one draw needn't show every extreme that they name: `live_blocks`: A supernode with 2^l * 8 block-rows (level l, listed level by level from level 0, by group within a level) has between a quarter of them (at least 1) and all of them live; the root supernode (the last entry) has all of them live. `diag_inverse`: each level's inverse diagonal block is lower triangular in its supernode's row order, with a positive diagonal.
All inputs are finite; a program needn't handle non-finite values.
Results may differ from the reference program's by a relative error of at most 0.009.
Values sent between devices are 32-bit elements; how exact they have to be, the bound alone decides.
No kernel may reach another device: no remote copies, remote signals or barrier semaphores. Data moves between devices by JAX's collectives and lax.ppermute only.
A program may use at most 128 MiB of HBM per device.

```python
import math
import jax
import jax.numpy as jnp
import numpy as np
from jax import lax

BS = 128
NRHS = 4
LEVELS = 3
ROWS = 4096
UCOLS = 10240
N_LEAF = 4
N_BLK = 8


def draw_diag_inverse(key, part):
    level_width = N_BLK * BS
    leaf_position = jnp.arange(N_LEAF).reshape(N_LEAF, 1, 1, 1)
    block_position = jnp.arange(N_BLK).reshape(1, N_BLK, 1, 1)
    row_position = jnp.arange(BS).reshape(1, 1, BS, 1)
    pieces = []
    for height in range(LEVELS):
        supernode_order = 2 ** height * level_width
        level_key = jax.random.fold_in(key, 11 + height)
        noise_key, scale_key = jax.random.split(level_key)
        full_shape = (N_LEAF, N_BLK, BS, supernode_order)
        jitter = jax.random.normal(noise_key, full_shape, jnp.float32)
        diagonal = jax.random.uniform(scale_key, (N_LEAF, N_BLK, BS, 1), jnp.float32, 0.6, 1.6)
        position = (leaf_position % 2 ** height * N_BLK + block_position) * BS + row_position
        column = jnp.arange(supernode_order).reshape(1, 1, 1, supernode_order)
        entries = jnp.where(column < position, jitter * (0.9 / math.sqrt(supernode_order)), jnp.where(column == position, diagonal, 0.0))
        pieces.append(entries)
    return jnp.concatenate(pieces, axis=3).astype(jnp.bfloat16)


def draw_live_blocks(key, part):
    lower_ends = []
    upper_ends = []
    for height in range(LEVELS):
        capacity = 2 ** height * N_BLK
        for group_number in range(N_LEAF // 2 ** height):
            lower_ends.append(max(1, capacity // 4))
            upper_ends.append(capacity + 1)
    lower_table = jnp.array(np.array(lower_ends, dtype=np.int32))
    upper_table = jnp.array(np.array(upper_ends, dtype=np.int32))
    drawn = jax.random.randint(key, (len(lower_ends),), lower_table, upper_table, jnp.int32)
    entry_index = jnp.arange(len(lower_ends)).astype(jnp.int32)
    return jnp.where(entry_index == len(lower_ends) - 1, upper_table - 1, drawn).astype(jnp.int32)


def level_of(key, extent, cuts, least, top_value):
    def one(dim, parts):
        steps = jax.random.uniform(jax.random.fold_in(jax.random.fold_in(key, 6), dim), (parts,), jnp.float32, least / len(cuts), top_value / len(cuts))
        return jnp.repeat(jnp.exp(steps), extent[dim] // parts).reshape((-1,) + (1,) * (len(extent) - dim - 1))

    level = one(*cuts[0])
    for cut in cuts[1:]:
        level = level * one(*cut)
    return level


def gaussian(own_key, shape, width, limit, shards=(), kind=jnp.bfloat16):
    values = width * jax.random.normal(own_key, shape, jnp.float32)
    if shards:
        values = values * level_of(own_key, shape, shards, -0.22, 0.18)
    return jnp.clip(values, -limit, limit).astype(kind)


def setup_inputs(seed: int = 0) -> dict:
    key_of = jax.random.split(jax.random.key(seed), 5)
    return {
        "right_side": gaussian(key_of[0], (NRHS, N_LEAF, N_BLK, LEVELS * BS), 1.0, 6.0, ((1, 4), (2, 8)), jnp.float32),
        "diag_inverse": draw_diag_inverse(jax.random.fold_in(key_of[4], 71), 0),
        "update_factor": gaussian(key_of[2], (N_LEAF, N_BLK, BS, UCOLS), ROWS ** -0.5, 0.09375, ((0, 4), (1, 8))),
        "live_blocks": draw_live_blocks(jax.random.fold_in(key_of[4], 71), 0),
    }


def grouped_product(vectors, matrices, contract_rows):
    vector_count = vectors.shape[0]
    groups = matrices.shape[0]
    stacked = vectors.reshape(vector_count, groups, -1).transpose(1, 0, 2)
    if contract_rows:
        dimension_numbers = (((1,), (0,)), ((), ()))
    else:
        dimension_numbers = (((1,), (1,)), ((), ()))

    def single(operands):
        return lax.dot_general(operands[0], operands[1], dimension_numbers, preferred_element_type=jnp.float32)

    result = lax.map(single, (stacked, matrices))
    return result.transpose(1, 0, 2).reshape(vector_count, -1)


def live_mask(live_blocks, height):
    leaf_position = jnp.arange(N_LEAF).astype(jnp.int32)[:, None]
    block_position = jnp.arange(N_BLK).astype(jnp.int32)[None, :]
    offset = 2 * N_LEAF - (2 * N_LEAF) // (2 ** height)
    counts = live_blocks[offset + leaf_position // (2 ** height)]
    alive = ((leaf_position % (2 ** height)) * N_BLK + block_position < counts).astype(jnp.float32)
    return jnp.broadcast_to(alive[:, :, None], (N_LEAF, N_BLK, BS)).reshape(ROWS)


def reference(right_side, diag_inverse, update_factor, live_blocks):
    level_width = N_BLK * BS
    orders = [(2 ** height) * level_width for height in range(LEVELS)]
    spans = [sum(orders[height + 1:]) for height in range(LEVELS)]
    update_start = [sum(spans[:height]) for height in range(LEVELS)]
    source_rows = right_side.reshape(NRHS, N_LEAF, N_BLK, LEVELS, BS)
    masks = [live_mask(live_blocks, height) for height in range(LEVELS)]

    def inverse_block(height):
        supernode_order = orders[height]
        start = (2 ** height - 1) * level_width
        return diag_inverse[:, :, :, start:start + supernode_order].reshape(N_LEAF // 2 ** height, supernode_order, supernode_order)

    def update_block(cursor, ancestor):
        ancestor_order = orders[ancestor]
        return update_factor[:, :, :, cursor:cursor + ancestor_order].reshape(N_LEAF // 2 ** ancestor, ancestor_order, ancestor_order)

    pending = [jnp.zeros((NRHS, ROWS), jnp.float32) for height in range(LEVELS)]
    forward = []
    for height in range(LEVELS):
        source = source_rows[:, :, :, height, :].reshape(NRHS, ROWS)
        reduced = (masks[height] * (source - pending[height])).astype(jnp.bfloat16)
        solved = masks[height] * grouped_product(reduced, inverse_block(height), False)
        forward.append(solved)
        rounded = solved.astype(jnp.bfloat16)
        cursor = update_start[height]
        for ancestor in range(height + 1, LEVELS):
            pending[ancestor] = pending[ancestor] + grouped_product(rounded, update_block(cursor, ancestor), True)
            cursor += orders[ancestor]

    gathered = [None] * LEVELS
    backward = [None] * LEVELS
    for height in reversed(range(LEVELS)):
        residual = forward[height]
        cursor = update_start[height]
        for ancestor in range(height + 1, LEVELS):
            residual = residual - grouped_product(gathered[ancestor], update_block(cursor, ancestor), False)
            cursor += orders[ancestor]
        weighted = (masks[height] * residual).astype(jnp.bfloat16)
        solved = masks[height] * grouped_product(weighted, inverse_block(height), True)
        backward[height] = solved
        gathered[height] = solved.astype(jnp.bfloat16)

    def arrange(levels_list):
        stacked = jnp.stack([item.reshape(NRHS, N_LEAF, N_BLK, BS) for item in levels_list], axis=3)
        return stacked.reshape(NRHS, N_LEAF, N_BLK, LEVELS * BS)

    return arrange(forward), arrange(backward)
```

```python
import jax
import jax.numpy as jnp
from jax import lax
from jax.sharding import PartitionSpec as P

BOTH = ("leaf", "blk")
LAST = (((1,), (1,)), ((), ()))
HALVE_BYTES = 65536


def moved(value, leaf_mask, block_mask):
    leaf_count = lax.axis_size("leaf")
    block_count = lax.axis_size("blk")
    route = []
    for leaf in range(leaf_count):
        for block in range(block_count):
            target = (leaf ^ leaf_mask) * block_count + (block ^ block_mask)
            route.append((leaf * block_count + block, target))
    return lax.ppermute(value, BOTH, route)


def parity():
    index = lax.axis_index("leaf") * lax.axis_size("blk") + lax.axis_index("blk")
    total = index
    for shift in (16, 8, 4, 2, 1):
        total = total ^ (total >> shift)
    return total & 1


def group_sum(value, height):
    block_bits = lax.axis_size("blk").bit_length() - 1
    moves = [(1 << bit | 1, 0) for bit in range(1, height)]
    moves += [(1, 1 << bit) for bit in range(block_bits)]
    if value.size * 4 < HALVE_BYTES:
        value = value + moved(value, 1, 0)
        for move in moves:
            value = value + moved(value, *move)
        return value
    half = value.shape[1] // 2
    odd = parity() == 1
    low, high = value[:, :half], value[:, half:]
    part = jnp.where(odd, high, low) + moved(jnp.where(odd, low, high), 1, 0)
    for move in moves:
        part = part + moved(part, *move)
    other = moved(part, 1, 0)
    return jnp.concatenate([jnp.where(odd, other, part), jnp.where(odd, part, other)], axis=1)


def local(right_side, diag_inverse, update_factor, live_blocks):
    leaf_count = lax.axis_size("leaf")
    block_count = lax.axis_size("blk")
    levels = leaf_count.bit_length()
    leaf_index = lax.axis_index("leaf")
    block_index = lax.axis_index("blk")
    block_rows = diag_inverse.shape[2]
    vectors = right_side.shape[0]
    level_width = block_count * block_rows
    inverse_rows = diag_inverse.reshape(block_rows, -1)
    update_rows = update_factor.reshape(block_rows, -1)
    side = right_side.reshape(vectors, levels * block_rows)
    orders = [(1 << height) * level_width for height in range(levels)]
    spans = [sum(orders[height + 1 :]) for height in range(levels)]
    own_positions, own_masks, group_masks, sides, inverses, updates = [], [], [], [], [], []
    for height in range(levels):
        offset = 2 * leaf_count - (2 * leaf_count >> height)
        live_count = live_blocks[offset + (leaf_index >> height)]
        position = (leaf_index & (1 << height) - 1) * block_count + block_index
        own_positions.append(position)
        own_masks.append((position < live_count).astype(jnp.float32))
        blocks = lax.broadcasted_iota(jnp.int32, (1, orders[height]), 1) // block_rows
        group_masks.append((blocks < live_count).astype(jnp.float32))
        sides.append(side[:, height * block_rows : (height + 1) * block_rows])
        start = ((1 << height) - 1) * level_width
        inverses.append(inverse_rows[:, start : start + orders[height]])
        cursor = sum(spans[:height])
        row = {}
        for ancestor in range(height + 1, levels):
            row[ancestor] = update_rows[:, cursor : cursor + orders[ancestor]]
            cursor += orders[ancestor]
        updates.append(row)

    def own_slot(height):
        blocks = lax.broadcasted_iota(jnp.int32, (1, orders[height]), 1) // block_rows
        tiled = jnp.tile(sides[height], (1, orders[height] // block_rows))
        return jnp.where(blocks == own_positions[height], tiled, 0.0)

    pending = [own_slot(height) for height in range(levels)]
    forward = []
    for height in range(levels):
        if height == 0:
            copies = jnp.broadcast_to(sides[0][None], (block_count, vectors, block_rows))
            source = lax.all_to_all(copies, "blk", 0, 0, tiled=True)
            source = source.transpose(1, 0, 2).reshape(vectors, level_width)
        else:
            source = group_sum(pending[height], height)
        reduced = (group_masks[height] * source).astype(jnp.bfloat16)
        solved = own_masks[height] * lax.dot_general(
            reduced, inverses[height], LAST, preferred_element_type=jnp.float32
        )
        forward.append(solved)
        rounded = solved.astype(jnp.bfloat16)
        for ancestor in range(height + 1, levels):
            pending[ancestor] = pending[ancestor] - jnp.dot(
                rounded, updates[height][ancestor], preferred_element_type=jnp.float32
            )
    residual = list(forward)
    backward = [None] * levels
    for height in reversed(range(levels)):
        weighted = (own_masks[height] * residual[height]).astype(jnp.bfloat16)
        partial = jnp.dot(weighted, inverses[height], preferred_element_type=jnp.float32)
        if height == 0:
            pieces = partial.reshape(vectors, block_count, block_rows).transpose(1, 0, 2)
            backward[0] = own_masks[0] * lax.all_to_all(pieces, "blk", 0, 0, tiled=True).sum(0)
            continue
        whole = group_masks[height] * group_sum(partial, height)
        backward[height] = lax.dynamic_slice_in_dim(
            whole, own_positions[height] * block_rows, block_rows, 1
        )
        rounded = whole.astype(jnp.bfloat16)
        for lower in range(height):
            residual[lower] = residual[lower] - lax.dot_general(
                rounded, updates[lower][height], LAST, preferred_element_type=jnp.float32
            )
    shape = (vectors, 1, 1, levels * block_rows)
    forward_out = jnp.concatenate(forward, axis=1).reshape(shape)
    backward_out = jnp.concatenate(backward, axis=1).reshape(shape)
    return (forward_out, backward_out)


def solution(mesh):
    in_specs = (
        P(None, "leaf", "blk", None),
        P("leaf", "blk", None, None),
        P("leaf", "blk", None, None),
        P(),
    )
    out_specs = (P(None, "leaf", "blk", None), P(None, "leaf", "blk", None))
    return jax.shard_map(local, mesh=mesh, in_specs=in_specs, out_specs=out_specs, check_vma=False)
```

```python
import functools

import jax
import jax.numpy as jnp
from jax import lax
from jax.experimental import pallas as pl
from jax.experimental.pallas import tpu as pltpu
from jax.sharding import PartitionSpec as P

BOTH = ("leaf", "blk")
LAST = (((1,), (1,)), ((), ()))
HALVE_BYTES = 65536
VMEM_LIMIT = 8 << 20
F32 = jnp.float32
BF16 = jnp.bfloat16


def moved(value, leaf_mask, block_mask):
    leaf_count = lax.axis_size("leaf")
    block_count = lax.axis_size("blk")
    route = []
    for leaf in range(leaf_count):
        for block in range(block_count):
            target = (leaf ^ leaf_mask) * block_count + (block ^ block_mask)
            route.append((leaf * block_count + block, target))
    return lax.ppermute(value, BOTH, route)


def group_moves(height):
    block_bits = lax.axis_size("blk").bit_length() - 1
    return [(1 << bit | 1, 0) for bit in range(1, height)] + [(1, 1 << bit) for bit in range(block_bits)]


def group_sum(values, height):
    if len(values) == 1:
        value = values[0] + moved(values[0], 1, 0)
        for move in group_moves(height):
            value = value + moved(value, *move)
        return (value,)
    part = values[0] + moved(values[1], 1, 0)
    for move in group_moves(height):
        part = part + moved(part, *move)
    return part, moved(part, 1, 0)


class Plan:
    def __init__(self, vectors, block_rows):
        self.leaf_count = lax.axis_size("leaf")
        self.block_count = lax.axis_size("blk")
        self.levels = self.leaf_count.bit_length()
        self.vectors = vectors
        self.rows = block_rows
        self.orders = [(1 << h) * self.block_count * block_rows for h in range(self.levels)]

    def halved(self, height):
        return height > 0 and self.orders[height] * self.vectors * 4 >= HALVE_BYTES

    def position(self, height):
        leaf = lax.axis_index("leaf") & (1 << height) - 1
        return leaf * self.block_count + lax.axis_index("blk")

    def odd(self):
        total = lax.axis_index("leaf") * self.block_count + lax.axis_index("blk")
        for shift in (16, 8, 4, 2, 1):
            total = total ^ (total >> shift)
        return total & 1

    def own_mask(self, lives_ref, height):
        return (self.position(height) < lives_ref[height]).astype(F32)

    def blocks(self, array):
        return [array[:, i : i + self.rows] for i in range(0, array.shape[1], self.rows)]

    def slotted(self, side, height, start, values):
        first = self.position(height) - start // self.rows
        ids = lax.broadcasted_iota(jnp.int32, side.shape, 1) * 0 + first
        parts = [jnp.where(ids == j, value + side, value) for j, value in enumerate(self.blocks(values))]
        return jnp.concatenate(parts, axis=1)

    def masked(self, lives_ref, height, source):
        if len(source) == 2:
            odd = jnp.full((self.vectors, self.rows), self.odd(), jnp.int32) == 1
            parts, others = self.blocks(source[0][...]), self.blocks(source[1][...])
            found = [jnp.where(odd, b, a) for a, b in zip(parts, others)]
            found += [jnp.where(odd, a, b) for a, b in zip(parts, others)]
        elif len(source[0].shape) == 3:
            found = [source[0][j] for j in range(self.block_count)]
        else:
            found = self.blocks(source[0][...])
        lives = lives_ref[height]
        return [jnp.where(lives > j, value, 0.0) for j, value in enumerate(found)]

    def spread_out(self, height):
        width = self.orders[height]
        if self.halved(height):
            return [(self.vectors, width // 2)] * 2
        return [(self.vectors, width)]

    def ranges(self, height):
        width = self.orders[height]
        if not self.halved(height):
            return [(0, width)]
        half = width // 2
        odd = self.odd()
        return [(pl.multiple_of(odd * half, half), half), (pl.multiple_of((1 - odd) * half, half), half)]


def call(body, name, outs, arguments):
    return pl.pallas_call(
        body,
        in_specs=[pl.BlockSpec(memory_space=pltpu.VMEM)] * len(arguments),
        out_specs=[pl.BlockSpec(memory_space=pltpu.VMEM)] * len(outs),
        out_shape=[pltpu.VMEM(shape, kind) for shape, kind in outs],
        compiler_params=pltpu.CompilerParams(vmem_limit_bytes=VMEM_LIMIT),
        name=name,
    )(*arguments)


def resident(inverse_rows, update_rows, inverse_cuts, update_cuts):
    cuts = [(0, *cut) for cut in inverse_cuts] + [(1, *cut) for cut in update_cuts]
    rows = inverse_rows.shape[2]

    def kernel(inverse_ref, update_ref, *rest):
        outs, sems = rest[: len(cuts)], rest[len(cuts)]
        copies = []
        for index, (which, start, width) in enumerate(cuts):
            source = (inverse_ref, update_ref)[which].at[0, 0, :, pl.ds(start, width)]
            copies.append(pltpu.make_async_copy(source, outs[index], sems.at[index]))
        for copy in copies:
            copy.start()
        for copy in copies:
            copy.wait()

    return pl.pallas_call(
        kernel,
        in_specs=[pl.BlockSpec(memory_space=pltpu.HBM)] * 2,
        out_specs=[pl.BlockSpec(memory_space=pltpu.VMEM)] * len(cuts),
        out_shape=[pltpu.VMEM((rows, width), inverse_rows.dtype) for _, _, width in cuts],
        scratch_shapes=[pltpu.SemaphoreType.DMA((len(cuts),))],
        compiler_params=pltpu.CompilerParams(vmem_limit_bytes=VMEM_LIMIT),
        name="resident",
    )(inverse_rows, update_rows)


def opening(plan, live, right_side):
    def kernel(live_hbm, side_hbm, copies_ref, pieces_ref, lives_ref, live_ref, side_ref, sems):
        fetch_side = pltpu.make_async_copy(side_hbm, side_ref, sems.at[0])
        fetch_live = pltpu.make_async_copy(live_hbm, live_ref, sems.at[1])
        fetch_side.start()
        fetch_live.start()
        fetch_side.wait()
        for height in range(plan.levels):
            columns = pl.ds(height * plan.rows, plan.rows)
            for vector in range(plan.vectors):
                pieces_ref[height, pl.ds(vector, 1), :] = side_ref[vector, 0, :, columns]
        for block in range(plan.block_count):
            copies_ref[block] = pieces_ref[0]
        fetch_live.wait()
        for height in range(plan.levels):
            offset = 2 * plan.leaf_count - (2 * plan.leaf_count >> height)
            count = live_ref[offset + (lax.axis_index("leaf") >> height)]
            lives_ref[height] = jnp.full((plan.vectors, plan.rows), count, jnp.int32)

    tile = (plan.vectors, plan.rows)
    levels = (plan.levels, *tile)
    outs = [((plan.block_count, *tile), F32), (levels, F32), (levels, jnp.int32)]
    return pl.pallas_call(
        kernel,
        in_specs=[pl.BlockSpec(memory_space=pltpu.HBM)] * 2,
        out_specs=[pl.BlockSpec(memory_space=pltpu.VMEM)] * len(outs),
        out_shape=[pltpu.VMEM(shape, kind) for shape, kind in outs],
        scratch_shapes=[
            pltpu.SMEM(live.shape, live.dtype),
            pltpu.VMEM(right_side.shape, F32),
            pltpu.SemaphoreType.DMA((2,)),
        ],
        compiler_params=pltpu.CompilerParams(vmem_limit_bytes=VMEM_LIMIT),
        name="opening",
    )(live, right_side)


def forward_step(plan, height, live, source, inverse, pieces, update, seed):
    top = height == plan.levels - 1
    above = height if top else height + 1
    count = len(source)

    def kernel(live_ref, *refs):
        source_refs = refs[:count]
        inverse_ref = refs[count]
        y_ref, outs = refs[-1 - len(plan.spread_out(above))], refs[-len(plan.spread_out(above)) :]
        reduced = jnp.concatenate(plan.masked(live_ref, height, source_refs), axis=1).astype(BF16)
        own = plan.own_mask(live_ref, height)
        solved = own * lax.dot_general(reduced, inverse_ref[...], LAST, preferred_element_type=F32)
        y_ref[...] = solved
        rounded = (own * solved).astype(BF16)
        for (start, width), out_ref in zip(plan.ranges(above), outs):
            columns = pl.ds(start, width)
            if top:
                out_ref[...] = jnp.dot(rounded, inverse_ref[:, columns], preferred_element_type=F32)
                continue
            pieces_ref, update_ref = refs[count + 1], refs[count + 2]
            product = jnp.dot(rounded, update_ref[:, columns], preferred_element_type=F32)
            total = -product if seed is None else -refs[count + 3][:, columns] - product
            out_ref[...] = plan.slotted(pieces_ref[above], above, start, total)

    arguments = [live, *source, inverse]
    if not top:
        arguments += [pieces, update] + ([] if seed is None else [seed])
    tile = (plan.vectors, plan.rows)
    outs = [(tile, F32)] + [(shape, F32) for shape in plan.spread_out(above)]
    return call(kernel, f"forward{height}", outs, arguments)


def seed_step(plan, live, solved, update, seed):
    def kernel(live_ref, solved_ref, update_ref, *rest):
        product = jnp.dot(solved_ref[...].astype(BF16), update_ref[...], preferred_element_type=F32)
        rest[-1][...] = product if seed is None else rest[0][...] + product

    arguments = [live, solved, update] + ([] if seed is None else [seed])
    return call(kernel, "seed", [((plan.vectors, update.shape[1]), F32)], arguments)[0]


def backward_step(plan, height, live, source, residual, update, inverse):
    above = height + 1
    count = len(source)
    tile = (plan.vectors, plan.rows)
    if height == 0:
        out_shapes = [(plan.block_count, *tile)]
    else:
        out_shapes = plan.spread_out(height)

    def kernel(live_ref, *refs):
        residual_ref, update_ref, inverse_ref = refs[count : count + 3]
        x_ref = refs[count + 3]
        outs = refs[count + 4 :]
        found = plan.masked(live_ref, above, refs[:count])
        rounded = jnp.concatenate(found, axis=1).astype(BF16)
        if height > 0:
            outs[-1][...] = rounded
        rest = residual_ref[...] - lax.dot_general(
            rounded, update_ref[...], LAST, preferred_element_type=F32
        )
        weighted = (plan.own_mask(live_ref, height) * rest).astype(BF16)
        if height == 0:
            product = jnp.dot(weighted, inverse_ref[...], preferred_element_type=F32)
            for block in range(plan.block_count):
                outs[0][block] = product[:, block * plan.rows : (block + 1) * plan.rows]
        else:
            for (start, width), out_ref in zip(plan.ranges(height), outs):
                out_ref[...] = jnp.dot(weighted, inverse_ref[:, pl.ds(start, width)], preferred_element_type=F32)
        ids = jnp.full((plan.vectors, plan.rows), plan.position(above), jnp.int32)
        total = found[0]
        for block in range(1, len(found)):
            total = jnp.where(ids == block, found[block], total)
        x_ref[...] = total

    outs = [(tile, F32)] + [(shape, F32) for shape in out_shapes]
    if height > 0:
        outs.append(((plan.vectors, plan.orders[above]), BF16))
    return call(kernel, f"backward{height}", outs, [live, *source, residual, update, inverse])


def residual_step(plan, live, residual, hat, update):
    def kernel(live_ref, residual_ref, hat_ref, update_ref, out_ref):
        out_ref[...] = residual_ref[...] - lax.dot_general(
            hat_ref[...], update_ref[...], LAST, preferred_element_type=F32
        )

    return call(kernel, "residual", [(residual.shape, F32)], [live, residual, hat, update])[0]


def closing(plan, live, partials, forward, backward):
    levels = plan.levels

    def kernel(live_ref, partial_ref, *refs):
        ys, xs = refs[:levels], refs[levels : 2 * levels - 1]
        forward_ref, backward_ref = refs[2 * levels - 1 :]
        total = partial_ref[0]
        for block in range(1, plan.block_count):
            total = total + partial_ref[block]
        lowest = plan.own_mask(live_ref, 0) * total
        for height in range(levels):
            columns = pl.ds(height * plan.rows, plan.rows)
            y = ys[height][...]
            x = lowest if height == 0 else xs[height - 1][...]
            for vector in range(plan.vectors):
                forward_ref[vector, 0, :, columns] = y[vector : vector + 1]
                backward_ref[vector, 0, :, columns] = x[vector : vector + 1]

    shape = jax.ShapeDtypeStruct((plan.vectors, 1, 1, levels * plan.rows), F32)
    arguments = [live, partials, *forward, *backward]
    return pl.pallas_call(
        kernel,
        in_specs=[pl.BlockSpec(memory_space=pltpu.VMEM)] * len(arguments),
        out_specs=[pl.BlockSpec(memory_space=pltpu.VMEM)] * 2,
        out_shape=[shape, shape],
        compiler_params=pltpu.CompilerParams(vmem_limit_bytes=VMEM_LIMIT),
        name="closing",
    )(*arguments)


def local(right_side, diag_inverse, update_factor, live):
    right_side, diag_inverse, update_factor, live = (
        pltpu.with_memory_space_constraint(array, pltpu.HBM)
        for array in (right_side, diag_inverse, update_factor, live)
    )
    block_rows = diag_inverse.shape[2]
    plan = Plan(right_side.shape[0], block_rows)
    levels, orders = plan.levels, plan.orders
    inverse_cuts, update_cuts, pairs = [], [], []
    cursor = 0
    for height in range(levels):
        inverse_cuts.append((sum(orders[:height]), orders[height]))
        for ancestor in range(height + 1, levels):
            pairs.append((ancestor, height))
            update_cuts.append((cursor, orders[ancestor]))
            cursor += orders[ancestor]
    copies, pieces, live = opening(plan, live, right_side)
    held = resident(diag_inverse, update_factor, inverse_cuts, update_cuts)
    inverses = held[:levels]
    updates = dict(zip(pairs, held[levels:]))

    source = (lax.all_to_all(copies, "blk", 0, 0, tiled=True),)
    forward = []
    seeds = {}
    for height in range(levels):
        solved, *sent = forward_step(
            plan, height, live, source, inverses[height], pieces,
            updates.get((height + 1, height)), seeds.get(height + 1),
        )
        forward.append(solved)
        source = group_sum(sent, min(height + 1, levels - 1))
        for ancestor in range(height + 2, levels):
            seeds[ancestor] = seed_step(plan, live, solved, updates[ancestor, height], seeds.get(ancestor))
    residuals = list(forward)
    backward = [None] * levels
    for height in reversed(range(levels - 1)):
        above = height + 1
        backward[above], *sent = backward_step(
            plan, height, live, source, residuals[height], updates[above, height], inverses[height]
        )
        hat = sent.pop() if height > 0 else None
        for lower in range(height):
            residuals[lower] = residual_step(plan, live, residuals[lower], hat, updates[above, lower])
        if height > 0:
            source = group_sum(sent, height)
    partials = lax.all_to_all(sent[0], "blk", 0, 0, tiled=True)
    return tuple(closing(plan, live, partials, forward, backward[1:]))


def solution(mesh):
    in_specs = (
        P(None, "leaf", "blk", None),
        P("leaf", "blk", None, None),
        P("leaf", "blk", None, None),
        P(),
    )
    out_specs = (P(None, "leaf", "blk", None), P(None, "leaf", "blk", None))
    return jax.shard_map(local, mesh=mesh, in_specs=in_specs, out_specs=out_specs, check_vma=False)
```

```python
import functools

import jax
import jax.numpy as jnp
from jax import lax
from jax.experimental import pallas as pl
from jax.experimental.pallas import tpu as pltpu
from jax.sharding import PartitionSpec as P

BOTH = ("leaf", "blk")
LAST = (((1,), (1,)), ((), ()))
HALVE_BYTES = 65536
VMEM_LIMIT = 8 << 20
FIRST = ((0, 0), (1, 0))
F32 = jnp.float32
BF16 = jnp.bfloat16


def moved(value, leaf_mask, block_mask):
    leaf_count = lax.axis_size("leaf")
    block_count = lax.axis_size("blk")
    route = []
    for leaf in range(leaf_count):
        for block in range(block_count):
            target = (leaf ^ leaf_mask) * block_count + (block ^ block_mask)
            route.append((leaf * block_count + block, target))
    return lax.ppermute(value, BOTH, route)


def group_steps(height):
    block_bits = lax.axis_size("blk").bit_length() - 1
    dimensions = [(1 << bit | 1, 0) for bit in range(1, height)] + [(1, 1 << bit) for bit in range(block_bits)]
    steps = [[dimensions.pop(1)]] if len(dimensions) % 2 else []
    return steps + [dimensions[i : i + 2] for i in range(0, len(dimensions), 2)]


def stepped(value, step):
    hops = list(step)
    if len(step) == 2:
        hops.append((step[0][0] ^ step[1][0], step[0][1] ^ step[1][1]))
    for part in [moved(value, *hop) for hop in hops]:
        value = value + part
    return value


def group_sum(values, height):
    total = values[0] + moved(values[-1], 1, 0)
    for step in group_steps(height):
        total = stepped(total, step)
    return (total,) if len(values) == 1 else (total, moved(total, 1, 0))


class Plan:
    def __init__(self, vectors, block_rows):
        self.leaf_count = lax.axis_size("leaf")
        self.block_count = lax.axis_size("blk")
        self.levels = self.leaf_count.bit_length()
        self.vectors = vectors
        self.rows = block_rows
        self.orders = [(1 << h) * self.block_count * block_rows for h in range(self.levels)]

    def halved(self, height):
        return height > 0 and self.orders[height] * self.vectors * 4 >= HALVE_BYTES

    def position(self, height):
        leaf = lax.axis_index("leaf") & (1 << height) - 1
        return leaf * self.block_count + lax.axis_index("blk")

    def odd(self):
        total = lax.axis_index("leaf") * self.block_count + lax.axis_index("blk")
        for shift in (16, 8, 4, 2, 1):
            total = total ^ (total >> shift)
        return total & 1

    def own_mask(self, lives_ref, height):
        return (self.position(height) < lives_ref[height]).astype(F32)

    def blocks(self, array):
        return [array[:, i : i + self.rows] for i in range(0, array.shape[1], self.rows)]

    def slotted(self, side, height, start, values):
        first = self.position(height) - start // self.rows
        ids = lax.broadcasted_iota(jnp.int32, side.shape, 1) * 0 + first
        parts = [jnp.where(ids == j, value + side, value) for j, value in enumerate(self.blocks(values))]
        return jnp.concatenate(parts, axis=1)

    def masked(self, lives_ref, height, source):
        if len(source) == 2:
            odd = jnp.full((self.vectors, self.rows), self.odd(), jnp.int32) == 1
            parts, others = self.blocks(source[0][...]), self.blocks(source[1][...])
            found = [jnp.where(odd, b, a) for a, b in zip(parts, others)]
            found += [jnp.where(odd, a, b) for a, b in zip(parts, others)]
        elif len(source[0].shape) == 3:
            found = [source[0][j] for j in range(self.block_count)]
        else:
            found = self.blocks(source[0][...])
        lives = lives_ref[height]
        return [jnp.where(lives > j, value, 0.0) for j, value in enumerate(found)]

    def spread_out(self, height):
        width = self.orders[height]
        if self.halved(height):
            return [(self.vectors, width // 2)] * 2
        return [(self.vectors, width)]

    def ranges(self, height):
        width = self.orders[height]
        if not self.halved(height):
            return [(0, width)]
        half = width // 2
        odd = self.odd()
        return [(pl.multiple_of(odd * half, half), half), (pl.multiple_of((1 - odd) * half, half), half)]


def call(body, name, outs, arguments):
    return pl.pallas_call(
        body,
        in_specs=[pl.BlockSpec(memory_space=pltpu.VMEM)] * len(arguments),
        out_specs=[pl.BlockSpec(memory_space=pltpu.VMEM)] * len(outs),
        out_shape=[pltpu.VMEM(shape, kind) for shape, kind in outs],
        compiler_params=pltpu.CompilerParams(vmem_limit_bytes=VMEM_LIMIT),
        name=name,
    )(*arguments)


def fetched(plan, cuts, refs, outs, sems):
    return [
        pltpu.make_async_copy(refs[which].at[0, 0, :, pl.ds(start, width)], out, sems.at[index])
        for index, ((which, start, width), out) in enumerate(zip(cuts, outs))
    ]


def resident(plan, diag_inverse, update_factor, cuts, after):
    count = len(cuts)

    def kernel(inverse_hbm, update_hbm, after_ref, *rest):
        copies = fetched(plan, cuts, (inverse_hbm, update_hbm), rest[:count], rest[count])
        for copy in copies:
            copy.start()
        for copy in copies:
            copy.wait()

    return pl.pallas_call(
        kernel,
        in_specs=[pl.BlockSpec(memory_space=pltpu.HBM)] * 2 + [pl.BlockSpec(memory_space=pltpu.VMEM)],
        out_specs=[pl.BlockSpec(memory_space=pltpu.VMEM)] * count,
        out_shape=[pltpu.VMEM((plan.rows, width), BF16) for _, _, width in cuts],
        scratch_shapes=[pltpu.SemaphoreType.DMA((count,))],
        compiler_params=pltpu.CompilerParams(vmem_limit_bytes=VMEM_LIMIT),
        name="resident",
    )(diag_inverse, update_factor, after)


def opening(plan, live, right_side, diag_inverse, update_factor, cuts):
    count = len(cuts)

    def kernel(live_hbm, side_hbm, inverse_hbm, update_hbm, copies_ref, pieces_ref, lives_ref, *rest):
        live_ref, side_ref, sems, held_sems = rest[count:]
        fetch_side = pltpu.make_async_copy(side_hbm, side_ref, sems.at[0])
        fetch_live = pltpu.make_async_copy(live_hbm, live_ref, sems.at[1])
        held = fetched(plan, cuts, (inverse_hbm, update_hbm), rest[:count], held_sems)
        fetch_side.start()
        fetch_live.start()
        for copy in held:
            copy.start()
        fetch_side.wait()
        for height in range(plan.levels):
            columns = pl.ds(height * plan.rows, plan.rows)
            for vector in range(plan.vectors):
                pieces_ref[height, pl.ds(vector, 1), :] = side_ref[vector, 0, :, columns]
        for block in range(plan.block_count):
            copies_ref[block] = pieces_ref[0]
        fetch_live.wait()
        for height in range(plan.levels):
            offset = 2 * plan.leaf_count - (2 * plan.leaf_count >> height)
            alive = live_ref[offset + (lax.axis_index("leaf") >> height)]
            lives_ref[height] = jnp.full((plan.vectors, plan.rows), alive, jnp.int32)
        for copy in held:
            copy.wait()

    tile = (plan.vectors, plan.rows)
    levels = (plan.levels, *tile)
    outs = [((plan.block_count, *tile), F32), (levels, F32), (levels, jnp.int32)]
    outs += [((plan.rows, width), BF16) for _, _, width in cuts]
    return pl.pallas_call(
        kernel,
        in_specs=[pl.BlockSpec(memory_space=pltpu.HBM)] * 4,
        out_specs=[pl.BlockSpec(memory_space=pltpu.VMEM)] * len(outs),
        out_shape=[pltpu.VMEM(shape, kind) for shape, kind in outs],
        scratch_shapes=[
            pltpu.SMEM(live.shape, live.dtype),
            pltpu.VMEM(right_side.shape, F32),
            pltpu.SemaphoreType.DMA((2,)),
            pltpu.SemaphoreType.DMA((count,)),
        ],
        compiler_params=pltpu.CompilerParams(vmem_limit_bytes=VMEM_LIMIT),
        name="opening",
    )(live, right_side, diag_inverse, update_factor)


def forward_step(plan, height, live, source, inverse, pieces, update, seed):
    top = height == plan.levels - 1
    above = height if top else height + 1
    count = len(source)

    def kernel(live_ref, *refs):
        source_refs = refs[:count]
        inverse_ref = refs[count]
        y_ref, outs = refs[-1 - len(plan.spread_out(above))], refs[-len(plan.spread_out(above)) :]
        reduced = jnp.concatenate(plan.masked(live_ref, height, source_refs), axis=1).astype(BF16)
        own = plan.own_mask(live_ref, height)
        solved = own * lax.dot_general(reduced, inverse_ref[...], LAST, preferred_element_type=F32)
        y_ref[...] = solved
        rounded = (own * solved).astype(BF16)
        for (start, width), out_ref in zip(plan.ranges(above), outs):
            columns = pl.ds(start, width)
            if top:
                out_ref[...] = jnp.dot(rounded, inverse_ref[:, columns], preferred_element_type=F32)
                continue
            pieces_ref, update_ref = refs[count + 1], refs[count + 2]
            product = jnp.dot(rounded, update_ref[:, columns], preferred_element_type=F32)
            total = -product if seed is None else -refs[count + 3][:, columns] - product
            out_ref[...] = plan.slotted(pieces_ref[above], above, start, total)

    arguments = [live, *source, inverse]
    if not top:
        arguments += [pieces, update] + ([] if seed is None else [seed])
    tile = (plan.vectors, plan.rows)
    outs = [(tile, F32)] + [(shape, F32) for shape in plan.spread_out(above)]
    return call(kernel, f"forward{height}", outs, arguments)


def seed_step(plan, live, solved, update, seed):
    def kernel(live_ref, solved_ref, update_ref, *rest):
        product = jnp.dot(solved_ref[...].astype(BF16), update_ref[...], preferred_element_type=F32)
        rest[-1][...] = product if seed is None else rest[0][...] + product

    arguments = [live, solved, update] + ([] if seed is None else [seed])
    return call(kernel, "seed", [((plan.vectors, update.shape[1]), F32)], arguments)[0]


def backward_step(plan, height, live, source, residual, update, inverse):
    above = height + 1
    count = len(source)
    tile = (plan.vectors, plan.rows)
    if height == 0:
        out_shapes = [(plan.block_count, *tile)]
    else:
        out_shapes = plan.spread_out(height)

    def kernel(live_ref, *refs):
        residual_ref, update_ref, inverse_ref = refs[count : count + 3]
        x_ref = refs[count + 3]
        outs = refs[count + 4 :]
        found = plan.masked(live_ref, above, refs[:count])
        rounded = jnp.concatenate(found, axis=1).astype(BF16)
        if height > 0:
            outs[-1][...] = rounded
        rest = residual_ref[...] - lax.dot_general(
            rounded, update_ref[...], LAST, preferred_element_type=F32
        )
        weighted = (plan.own_mask(live_ref, height) * rest).astype(BF16)
        if height == 0:
            product = jnp.dot(weighted, inverse_ref[...], preferred_element_type=F32)
            for block in range(plan.block_count):
                outs[0][block] = product[:, block * plan.rows : (block + 1) * plan.rows]
        else:
            for (start, width), out_ref in zip(plan.ranges(height), outs):
                out_ref[...] = jnp.dot(weighted, inverse_ref[:, pl.ds(start, width)], preferred_element_type=F32)
        ids = jnp.full((plan.vectors, plan.rows), plan.position(above), jnp.int32)
        total = found[0]
        for block in range(1, len(found)):
            total = jnp.where(ids == block, found[block], total)
        x_ref[...] = total

    outs = [(tile, F32)] + [(shape, F32) for shape in out_shapes]
    if height > 0:
        outs.append(((plan.vectors, plan.orders[above]), BF16))
    return call(kernel, f"backward{height}", outs, [live, *source, residual, update, inverse])


def residual_step(plan, live, residual, hat, update):
    def kernel(live_ref, residual_ref, hat_ref, update_ref, out_ref):
        out_ref[...] = residual_ref[...] - lax.dot_general(
            hat_ref[...], update_ref[...], LAST, preferred_element_type=F32
        )

    return call(kernel, "residual", [(residual.shape, F32)], [live, residual, hat, update])[0]


def closing(plan, live, partials, forward, backward):
    levels = plan.levels

    def kernel(live_ref, partial_ref, *refs):
        ys, xs = refs[:levels], refs[levels : 2 * levels - 1]
        forward_ref, backward_ref = refs[2 * levels - 1 :]
        total = partial_ref[0]
        for block in range(1, plan.block_count):
            total = total + partial_ref[block]
        lowest = plan.own_mask(live_ref, 0) * total
        for height in range(levels):
            columns = pl.ds(height * plan.rows, plan.rows)
            y = ys[height][...]
            x = lowest if height == 0 else xs[height - 1][...]
            for vector in range(plan.vectors):
                forward_ref[vector, 0, :, columns] = y[vector : vector + 1]
                backward_ref[vector, 0, :, columns] = x[vector : vector + 1]

    shape = jax.ShapeDtypeStruct((plan.vectors, 1, 1, levels * plan.rows), F32)
    arguments = [live, partials, *forward, *backward]
    return pl.pallas_call(
        kernel,
        in_specs=[pl.BlockSpec(memory_space=pltpu.VMEM)] * len(arguments),
        out_specs=[pl.BlockSpec(memory_space=pltpu.VMEM)] * 2,
        out_shape=[shape, shape],
        compiler_params=pltpu.CompilerParams(vmem_limit_bytes=VMEM_LIMIT),
        name="closing",
    )(*arguments)


def local(right_side, diag_inverse, update_factor, live):
    right_side, diag_inverse, update_factor, live = (
        pltpu.with_memory_space_constraint(array, pltpu.HBM)
        for array in (right_side, diag_inverse, update_factor, live)
    )
    block_rows = diag_inverse.shape[2]
    plan = Plan(right_side.shape[0], block_rows)
    levels, orders = plan.levels, plan.orders
    cuts = {(height, height): (0, sum(orders[:height]), orders[height]) for height in range(levels)}
    cursor = 0
    for height in range(levels):
        for ancestor in range(height + 1, levels):
            cuts[ancestor, height] = (1, cursor, orders[ancestor])
            cursor += orders[ancestor]
    first = [key for key in cuts if key in FIRST]
    later = [key for key in cuts if key not in FIRST]
    copies, pieces, live, *held = opening(
        plan, live, right_side, diag_inverse, update_factor, [cuts[key] for key in first]
    )
    matrices = dict(zip(first, held))
    source = (lax.all_to_all(copies, "blk", 0, 0, tiled=True),)
    forward = []
    seeds = {}
    for height in range(levels):
        solved, *sent = forward_step(
            plan, height, live, source, matrices[height, height], pieces,
            matrices.get((height + 1, height)), seeds.get(height + 1),
        )
        forward.append(solved)
        if height == 0:
            held = resident(plan, diag_inverse, update_factor, [cuts[key] for key in later], solved)
            matrices.update(zip(later, held))
        source = group_sum(sent, min(height + 1, levels - 1))
        for ancestor in range(height + 2, levels):
            seeds[ancestor] = seed_step(plan, live, solved, matrices[ancestor, height], seeds.get(ancestor))
    residuals = list(forward)
    backward = [None] * levels
    for height in reversed(range(levels - 1)):
        above = height + 1
        backward[above], *sent = backward_step(
            plan, height, live, source, residuals[height], matrices[above, height], matrices[height, height]
        )
        hat = sent.pop() if height > 0 else None
        for lower in range(height):
            residuals[lower] = residual_step(plan, live, residuals[lower], hat, matrices[above, lower])
        if height > 0:
            source = group_sum(sent, height)
    partials = lax.all_to_all(sent[0], "blk", 0, 0, tiled=True)
    return tuple(closing(plan, live, partials, forward, backward[1:]))


def solution(mesh):
    in_specs = (
        P(None, "leaf", "blk", None),
        P("leaf", "blk", None, None),
        P("leaf", "blk", None, None),
        P(),
    )
    out_specs = (P(None, "leaf", "blk", None), P(None, "leaf", "blk", None))
    return jax.shard_map(local, mesh=mesh, in_specs=in_specs, out_specs=out_specs, check_vma=False)
```
